32 devices in a mesh: dp: 8 (over z, x), seq: 4 (over y, core).
Axes of the slice: x: 2, y: 2, z: 4, core: 2. Of those that a mesh axis runs over, the one named last changes fastest.
Arguments:
- hidden: bfloat16 [8, 4096, 4096], P('dp', 'seq'), may hold values from -6 to 6
- value_weight: bfloat16 [4096, 64], replicated, may hold values from -0.09375 to 0.09375
- value_bias: float32 [64], replicated, may hold values from -1 to 1
- returns: float32 [8, 4096], P('dp', 'seq'), may hold values from -12 to 12, as said below
- task_bins: int32 [8, 4096], P('dp', 'seq'), may hold values from 0 to 63
- loss_mask: int32 [8, 4096], P('dp', 'seq'), may hold values 0 or 1
Outputs:
- targets: float32 [8, 4096], P('dp', 'seq')
- weight_grad: float32 [4096, 64], replicated
- bias_grad: float32 [64], replicated
The draws below stay inside these ranges and needn't reach their ends.
Inputs may be any that keep to these rules, and one draw needn't show every extreme that they name: The returns of one rollout share a level and a trend along positions.
All inputs are finite; a program needn't handle non-finite values.
Results may differ from the reference program's by a relative error of at most 0.00083.
Values sent between devices are 32-bit elements.
No kernel may reach another device: no remote copies, remote signals or barrier semaphores. Data moves between devices by JAX's collectives and lax.ppermute only.
A program may use at most 64 MiB of HBM per device.

```python
import math
import jax
import jax.numpy as jnp
import numpy as np
from jax import lax

D = 4096
NB = 64
ROLLOUTS = 8
LENGTH = 4096


def draw_returns(key, part):
    keys = jax.random.split(key, 4)
    level = jax.random.uniform(keys[0], (ROLLOUTS, 1), jnp.float32, -3.0, 3.0)
    noise = jnp.clip(jax.random.normal(keys[2], (ROLLOUTS, LENGTH), jnp.float32), -3.0, 3.0)
    trend = jax.random.uniform(keys[1], (ROLLOUTS, 1), jnp.float32, -2.0, 2.0)
    spread = jnp.exp(jax.random.uniform(keys[3], (ROLLOUTS, 1), jnp.float32, math.log(0.5), math.log(2.0)))
    position = jnp.arange(LENGTH, dtype=jnp.float32) / LENGTH
    return level + trend * position[None, :] + noise * spread


def plant(result, key, smallest, largest):
    extent = result.shape
    spot = [jax.random.randint(jax.random.fold_in(key, axis), (), 0, extent[axis]) for axis in range(len(extent))]
    result = result.at[tuple(spot)].set(smallest)
    longest = extent.index(max(extent))
    spot[longest] = (spot[longest] + 1) % extent[longest]
    return result.at[tuple(spot)].set(largest)


def steps_of(own_key, extent, shards, low, largest):
    factor_of, own = 1.0, jax.random.fold_in(own_key, 6)
    for axis_at, shards_of in shards:
        heights = jnp.exp(jax.random.uniform(jax.random.fold_in(own, axis_at), (shards_of,), jnp.float32, low / len(shards), largest / len(shards)))
        factor_of = factor_of * jnp.repeat(heights, extent[axis_at] // shards_of).reshape([-1 if axis == axis_at else 1 for axis in range(len(extent))])
    return factor_of


def cumulative_ranks(number_of, skew):
    weights = [(1 << 20) // math.isqrt(grade ** skew) + 1 for grade in range(1, number_of + 1)]
    scale = 1 + sum(weights) // (1 << 30)
    return np.cumsum(np.array([max(1, weight // scale) for weight in weights]))


def skewed_ids(key, shape, number_of, skew):
    grid = cumulative_ranks(number_of, skew)
    pick = jax.random.randint(jax.random.fold_in(key, 1), shape, 0, int(grid[number_of - 1]))
    grade = jnp.searchsorted(jnp.asarray(grid, jnp.int32), pick, side="right")
    return jax.random.permutation(jax.random.fold_in(key, 2), number_of)[grade].astype(jnp.int32)


def centred(own_key, extent, scale, most, shards=(), kind=jnp.bfloat16):
    drawn = scale * jax.random.normal(own_key, extent, jnp.float32)
    if shards:
        drawn = drawn * steps_of(own_key, extent, shards, -0.22, 0.18)
    return jnp.clip(drawn, -most, most).astype(kind)


def setup_inputs(seed: int = 0) -> dict:
    arg_keys = jax.random.split(jax.random.key(seed), 7)
    hidden = centred(arg_keys[0], (ROLLOUTS, LENGTH, D), 1.0, 6.0, ((0, 8), (1, 4)))
    value_weight = centred(arg_keys[1], (D, NB), D ** -0.5, 0.09375)
    value_bias = jnp.clip(jax.random.uniform(arg_keys[2], (NB,), jnp.float32, -1.0, 1.0), -1.0, 1.0)
    returns = draw_returns(jax.random.fold_in(arg_keys[6], 71), 0)
    task_bins = plant(skewed_ids(arg_keys[4], (ROLLOUTS, LENGTH), NB, 2), jax.random.fold_in(arg_keys[4], 3), 0, NB - 1).astype(jnp.int32)
    loss_mask = plant((jax.random.randint(arg_keys[5], (ROLLOUTS, LENGTH), 0, 4) < 3).astype(jnp.int32), jax.random.fold_in(arg_keys[5], 1), 0, 1)
    return {"hidden": hidden, "value_weight": value_weight, "value_bias": value_bias, "returns": returns, "task_bins": task_bins, "loss_mask": loss_mask}


def reference(hidden, value_weight, value_bias, returns, task_bins, loss_mask):
    bins_iota = jnp.arange(NB, dtype=jnp.int32)
    chosen = (task_bins[..., None] == bins_iota).astype(jnp.float32)
    onehot = chosen * loss_mask[..., None].astype(jnp.float32)
    counts = lax.optimization_barrier(jnp.sum(onehot, axis=(0, 1)))
    floor_counts = jnp.maximum(counts, 1.0)
    means = lax.optimization_barrier(jnp.sum(onehot * returns[..., None], axis=(0, 1))) / floor_counts
    deviation = returns[..., None] - means
    second = lax.optimization_barrier(jnp.sum(onehot * deviation * deviation, axis=(0, 1)))
    spread = jnp.sqrt(second / floor_counts + 0.1)
    targets = lax.optimization_barrier(jnp.sum(chosen * (deviation / spread), axis=-1))

    def rollout_step(running, slices):
        states, target_row, chosen_row, valid = slices
        scores = jnp.dot(states, value_weight, preferred_element_type=jnp.float32)
        predicted = lax.optimization_barrier(jnp.sum((scores + value_bias) * chosen_row, axis=-1))
        slope = valid * jnp.clip(predicted - target_row, -1.0, 1.0) / ROLLOUTS
        coefficient = chosen_row * slope[:, None]
        weight_part = lax.dot_general(states, coefficient.astype(jnp.bfloat16), (((0,), (0,)), ((), ())), preferred_element_type=jnp.float32)
        return ((running[0] + weight_part, running[1] + lax.optimization_barrier(jnp.sum(coefficient, axis=0))), None)
    start = (jnp.zeros((D, NB), jnp.float32), jnp.zeros((NB,), jnp.float32))
    (weight_grad, bias_grad), unused = lax.scan(rollout_step, start, (hidden, targets, chosen, loss_mask.astype(jnp.float32)))
    return (targets, weight_grad, bias_grad)
```

```python
import jax
import jax.numpy as jnp
from jax import lax
from jax.sharding import PartitionSpec as P

LANES = 128
SUBLANES = 8


def exchange_rounds(sizes):
    rounds = []
    for axis, widest in (("seq", 2), ("dp", 4)):
        stride, left = 1, sizes[axis]
        while left > 1:
            wanted = 2 if stride == 1 else widest
            radix = next(r for r in [wanted, 2] + list(range(3, left + 1)) if left % r == 0)
            rounds.append((axis, stride, radix))
            stride, left = stride * radix, left // radix
    return rounds


def shift(value, axis, stride, radix, by):
    pairs = []
    for source in range(lax.axis_size(axis)):
        digit = (source // stride) % radix
        pairs.append((source, source + ((digit + by) % radix - digit) * stride))
    return lax.ppermute(value, axis, pairs)


def sum_small(value, rounds):
    for axis, stride, radix in rounds:
        pieces = [shift(value, axis, stride, radix, by) for by in range(1, radix)]
        for piece in pieces:
            value = value + piece
    return value


def binary(rounds, sizes):
    split = []
    for axis, stride, radix in rounds:
        while radix % 2 == 0 and radix > 2:
            split.append((axis, stride, 2))
            stride, radix = stride * 2, radix // 2
        split.append((axis, stride, radix))
    return split


def digit_of(axis, stride, radix):
    return (lax.axis_index(axis) // stride) % radix


def scatter_sum(tiles, extra, rounds):
    for axis, stride, radix in rounds:
        mine = digit_of(axis, stride, radix)
        count = tiles.shape[0] // radix
        got = []
        for by in range(1, radix):
            part = lax.dynamic_slice_in_dim(tiles, ((mine + by) % radix) * count, count, 0)
            got.append(shift(jnp.concatenate([part, extra], axis=0), axis, stride, radix, by))
        tiles = lax.dynamic_slice_in_dim(tiles, mine * count, count, 0)
        for piece in got:
            tiles = tiles + piece[:count]
            extra = extra + piece[count:]
    return tiles, extra


def gather(tiles, rounds):
    for axis, stride, radix in reversed(rounds):
        mine = digit_of(axis, stride, radix)
        count = tiles.shape[0]
        got = [shift(tiles, axis, stride, radix, by) for by in range(1, radix)]
        whole = jnp.zeros((count * radix,) + tiles.shape[1:], tiles.dtype)
        whole = lax.dynamic_update_slice_in_dim(whole, tiles, mine * count, 0)
        for by in range(1, radix):
            whole = lax.dynamic_update_slice_in_dim(whole, got[by - 1], ((mine - by) % radix) * count, 0)
        tiles = whole
    return tiles


def on_device(hidden, value_weight, value_bias, returns, task_bins, loss_mask):
    sizes = {axis: lax.axis_size(axis) for axis in ("dp", "seq")}
    rounds = exchange_rounds(sizes)
    rollouts = hidden.shape[0] * sizes["dp"]
    width, tasks = value_weight.shape
    states = hidden.reshape(-1, width)
    flat_returns = returns.reshape(-1)
    bins_iota = jnp.arange(tasks, dtype=jnp.int32)
    chosen = (task_bins.reshape(-1)[:, None] == bins_iota).astype(jnp.float32)
    valid = loss_mask.reshape(-1).astype(jnp.float32)
    onehot = chosen * valid[:, None]
    counts = jnp.sum(onehot, axis=0)
    summed = jnp.sum(onehot * flat_returns[:, None], axis=0)
    squares = jnp.sum(onehot * flat_returns[:, None] * flat_returns[:, None], axis=0)
    counts, summed, squares = sum_small(jnp.stack([counts, summed, squares]), binary(rounds, sizes))
    scores = jnp.dot(states, value_weight, preferred_element_type=jnp.float32)
    predicted = jnp.sum((scores + value_bias) * chosen, axis=-1)
    floor_counts = jnp.maximum(counts, 1.0)
    means = summed / floor_counts
    second = squares - summed * means
    spread = jnp.sqrt(second / floor_counts + 0.1)
    deviation = flat_returns[:, None] - means
    targets = jnp.sum(chosen * (deviation / spread), axis=-1)
    slope = valid * jnp.clip(predicted - targets, -1.0, 1.0) / rollouts
    coefficient = chosen * slope[:, None]
    weight_grad = lax.dot_general(
        coefficient.astype(jnp.bfloat16),
        states,
        (((0,), (0,)), ((), ())),
        preferred_element_type=jnp.float32,
    )
    bias_grad = jnp.sum(coefficient, axis=0)
    up, across = tasks // SUBLANES, width // LANES
    tiles = weight_grad.reshape(up, SUBLANES, across, LANES).transpose(0, 2, 1, 3)
    tiles = tiles.reshape(up * across, SUBLANES, LANES)
    extra = jnp.zeros((SUBLANES, LANES), jnp.float32).at[0, :tasks].set(bias_grad)[None]
    tiles, extra = scatter_sum(tiles, extra, rounds)
    tiles = gather(tiles, rounds)
    weight_grad = tiles.reshape(up, across, SUBLANES, LANES).transpose(0, 2, 1, 3)
    weight_grad = weight_grad.reshape(tasks, width).T
    return (targets.reshape(returns.shape), weight_grad, extra[0, 0, :tasks])


def solution(mesh):
    placed = (P("dp", "seq", None), P(), P(), P("dp", "seq"), P("dp", "seq"), P("dp", "seq"))
    return jax.shard_map(
        on_device, mesh=mesh, in_specs=placed, out_specs=(P("dp", "seq"), P(), P()), check_vma=False
    )
```

```python
import jax
import jax.numpy as jnp
from jax import lax
from jax.sharding import PartitionSpec as P

LANES = 128
SUBLANES = 8
AXES = ("dp", "seq")


def factor(left, widest):
    return next(r for r in [widest, 2] + list(range(3, left + 1)) if left % r == 0)


def small_rounds(total):
    rounds, stride = [], 1
    while stride < total:
        radix = factor(total // stride, 2)
        rounds.append((stride, radix))
        stride *= radix
    return rounds


def wide_rounds(dp, seq):
    rounds = []
    for first, left, plan in ((1, seq, (2, 2)), (seq, dp, (2, 4))):
        stride, at = first, 0
        while left > 1:
            radix = factor(left, plan[min(at, 1)])
            rounds.append((stride, radix))
            stride, left, at = stride * radix, left // radix, at + 1
    paired = [((stride, stride), radix) for stride, radix in rounds]
    ahead = [at for at, (stride, radix) in enumerate(rounds) if stride == seq]
    if len(rounds) > 2 and rounds[0] == (1, 2) and seq > 2 and ahead:
        one, other = rounds[1], rounds[ahead[0]]
        if one[1] == other[1] and one[0] != other[0]:
            paired[1] = ((one[0], other[0]), one[1])
            paired[ahead[0]] = ((other[0], one[0]), one[1])
            paired.insert(2, paired.pop(ahead[0]))
    return paired


def shift(value, strides, radix, by):
    pairs = []
    for source in range(lax.axis_size(AXES)):
        stride = strides[source % 2]
        digit = (source // stride) % radix
        pairs.append((source, source + ((digit + by) % radix - digit) * stride))
    return lax.ppermute(value, AXES, pairs)


def digit_of(strides, radix):
    here = lax.axis_index(AXES)
    stride = jnp.where(here % 2 == 0, strides[0], strides[1])
    return (here // stride) % radix


def scatter_sum(tiles, extra, rounds):
    for strides, radix in rounds:
        mine = digit_of(strides, radix)
        count = tiles.shape[0] // radix
        got = []
        for by in range(1, radix):
            part = lax.dynamic_slice_in_dim(tiles, ((mine + by) % radix) * count, count, 0)
            got.append(shift(jnp.concatenate([part, extra], axis=0), strides, radix, by))
        tiles = lax.dynamic_slice_in_dim(tiles, mine * count, count, 0)
        for piece in got:
            tiles = tiles + piece[:count]
            extra = extra + piece[count:]
    return tiles, extra


def gather(tiles, rounds):
    for strides, radix in reversed(rounds):
        mine = digit_of(strides, radix)
        count = tiles.shape[0]
        got = [shift(tiles, strides, radix, by) for by in range(1, radix)]
        whole = jnp.zeros((count * radix,) + tiles.shape[1:], tiles.dtype)
        whole = lax.dynamic_update_slice_in_dim(whole, tiles, mine * count, 0)
        for by in range(1, radix):
            whole = lax.dynamic_update_slice_in_dim(whole, got[by - 1], ((mine - by) % radix) * count, 0)
        tiles = whole
    return tiles


def on_device(hidden, value_weight, value_bias, returns, task_bins, loss_mask):
    dp, seq = lax.axis_size("dp"), lax.axis_size("seq")
    rounds = wide_rounds(dp, seq)
    rollouts = hidden.shape[0] * dp
    width, tasks = value_weight.shape
    states = hidden.reshape(-1, width)
    flat_returns = returns.reshape(-1)
    bins = task_bins.reshape(-1)
    bins_iota = jnp.arange(tasks, dtype=jnp.int32)
    onehot = (bins[:, None] == bins_iota) & (loss_mask.reshape(-1)[:, None] != 0)
    counts = jnp.sum(jnp.where(onehot, 1.0, 0.0), axis=0)
    summed = jnp.sum(jnp.where(onehot, flat_returns[:, None], 0.0), axis=0)
    squares = jnp.sum(jnp.where(onehot, flat_returns[:, None] * flat_returns[:, None], 0.0), axis=0)
    stats = jnp.stack([counts, summed, squares])
    chosen = (bins[:, None] == bins_iota).astype(jnp.float32)
    half = states.shape[0] // 2
    pieces = []
    for at, (stride, radix) in enumerate(small_rounds(dp * seq)):
        got = [shift(stats, (stride, stride), radix, by) for by in range(1, radix)]
        if at in (1, 2):
            rows = slice(0, half) if at == 1 else slice(half, None)
            bias, stats = lax.optimization_barrier((value_bias, stats))
            scores = jnp.dot(states[rows], value_weight, preferred_element_type=jnp.float32)
            picked = jnp.sum((scores + bias) * chosen[rows], axis=-1)
            got, picked = lax.optimization_barrier((got, picked))
            pieces.append(picked)
        for piece in got:
            stats = stats + piece
    predicted = jnp.concatenate(pieces)
    counts, summed, squares = stats
    floor_counts = jnp.maximum(counts, 1.0)
    means = summed / floor_counts
    second = squares - summed * means
    spread = jnp.sqrt(second / floor_counts + 0.1)
    deviation = flat_returns[:, None] - means
    targets = jnp.sum(chosen * (deviation / spread), axis=-1)
    valid = loss_mask.reshape(-1).astype(jnp.float32)
    slope = valid * jnp.clip(predicted - targets, -1.0, 1.0) / rollouts
    coefficient = chosen * slope[:, None]
    weight_grad = lax.dot_general(
        states,
        coefficient.astype(jnp.bfloat16),
        (((0,), (0,)), ((), ())),
        preferred_element_type=jnp.float32,
    )
    weight_grad = lax.optimization_barrier(weight_grad).T
    bias_grad = jnp.sum(coefficient, axis=0)
    up, across = tasks // SUBLANES, width // LANES
    tiles = weight_grad.reshape(up, SUBLANES, across, LANES).transpose(0, 2, 1, 3)
    tiles = tiles.reshape(up * across, SUBLANES, LANES)
    extra = jnp.zeros((SUBLANES, LANES), jnp.float32).at[0, :tasks].set(bias_grad)[None]
    tiles, extra = scatter_sum(tiles, extra, rounds)
    tiles = gather(tiles, rounds)
    weight_grad = tiles.reshape(up, across, SUBLANES, LANES).transpose(0, 2, 1, 3)
    weight_grad = weight_grad.reshape(tasks, width).T
    return (targets.reshape(returns.shape), weight_grad, extra[0, 0, :tasks])


def solution(mesh):
    placed = (P("dp", "seq", None), P(), P(), P("dp", "seq"), P("dp", "seq"), P("dp", "seq"))
    return jax.shard_map(
        on_device, mesh=mesh, in_specs=placed, out_specs=(P("dp", "seq"), P(), P()), check_vma=False
    )
```

```python
import jax
import jax.numpy as jnp
from jax import lax
from jax.experimental import pallas as pl
from jax.sharding import PartitionSpec as P

LANES = 128
SUBLANES = 8
AXES = ("dp", "seq")


def factor(left, widest):
    return next(r for r in [widest, 2] + list(range(3, left + 1)) if left % r == 0)


def small_rounds(total):
    rounds, stride = [], 1
    while stride < total:
        radix = factor(total // stride, 2)
        rounds.append((stride, radix))
        stride *= radix
    return rounds


def wide_rounds(dp, seq):
    rounds = []
    for first, left, plan in ((1, seq, (2, 2)), (seq, dp, (2, 4))):
        stride, at = first, 0
        while left > 1:
            radix = factor(left, plan[min(at, 1)])
            rounds.append((stride, radix))
            stride, left, at = stride * radix, left // radix, at + 1
    paired = [((stride, stride), radix) for stride, radix in rounds]
    ahead = [at for at, (stride, radix) in enumerate(rounds) if stride == seq]
    if len(rounds) > 2 and rounds[0] == (1, 2) and seq > 2 and ahead:
        one, other = rounds[1], rounds[ahead[0]]
        if one[1] == other[1] and one[0] != other[0]:
            paired[1] = ((one[0], other[0]), one[1])
            paired[ahead[0]] = ((other[0], one[0]), one[1])
            paired.insert(2, paired.pop(ahead[0]))
    return paired


def shift(value, strides, radix, by):
    pairs = []
    for source in range(lax.axis_size(AXES)):
        stride = strides[source % 2]
        digit = (source // stride) % radix
        pairs.append((source, source + ((digit + by) % radix - digit) * stride))
    return lax.ppermute(value, AXES, pairs)


def digit_of(strides, radix):
    here = lax.axis_index(AXES)
    stride = jnp.where(here % 2 == 0, strides[0], strides[1])
    return (here // stride) % radix


def scatter_round(tiles, extra, strides, radix):
    mine = digit_of(strides, radix)
    count = tiles.shape[0] // radix
    got = []
    for by in range(1, radix):
        part = lax.dynamic_slice_in_dim(tiles, ((mine + by) % radix) * count, count, 0)
        part = part if extra is None else jnp.concatenate([part, extra], axis=0)
        got.append(shift(part, strides, radix, by))
    tiles = lax.dynamic_slice_in_dim(tiles, mine * count, count, 0)
    for piece in got:
        tiles = tiles + piece[:count]
        extra = None if extra is None else extra + piece[count:]
    return tiles, extra


def gather_round(tiles, strides, radix):
    mine = digit_of(strides, radix)
    count = tiles.shape[0]
    got = [shift(tiles, strides, radix, by) for by in range(1, radix)]
    whole = jnp.zeros((count * radix,) + tiles.shape[1:], tiles.dtype)
    whole = lax.dynamic_update_slice_in_dim(whole, tiles, mine * count, 0)
    for by in range(1, radix):
        whole = lax.dynamic_update_slice_in_dim(whole, got[by - 1], ((mine - by) % radix) * count, 0)
    return whole


def all_sum(chains, extra, rounds):
    apart = min(3, len(rounds)) if len(chains) > 1 else 0
    extras = [None] * (len(chains) - 1) + [extra]
    for strides, radix in rounds[:apart]:
        both = [scatter_round(tiles, more, strides, radix) for tiles, more in zip(chains, extras)]
        chains, extras = [one[0] for one in both], [one[1] for one in both]
    extra = extras[-1]
    count = chains[0].shape[0]
    tiles = jnp.concatenate(chains, axis=0)
    for strides, radix in rounds[apart:]:
        tiles, extra = scatter_round(tiles, extra, strides, radix)
    for strides, radix in reversed(rounds[apart:]):
        tiles = gather_round(tiles, strides, radix)
    chains = [tiles[at * count:(at + 1) * count] for at in range(len(chains))]
    for strides, radix in reversed(rounds[:apart]):
        chains = [gather_round(tiles, strides, radix) for tiles in chains]
    return chains, extra


def stats_kernel(returns_ref, bins_ref, mask_ref, out_ref):
    rows, tasks = out_ref.shape
    tokens = returns_ref.shape[1]
    value = returns_ref[...]
    task = lax.broadcasted_iota(jnp.int32, (tasks, tokens), 0)
    onehot = (task == bins_ref[...]) & (mask_ref[...] != 0)
    row = lax.broadcasted_iota(jnp.int32, (rows, tokens), 0)
    terms = jnp.where(row == 0, 1.0, jnp.where(row == 1, value, jnp.where(row == 2, value * value, 0.0)))
    out_ref[...] = lax.dot_general(
        terms,
        jnp.where(onehot, 1.0, 0.0),
        (((1,), (1,)), ((), ())),
        precision=lax.Precision.HIGHEST,
        preferred_element_type=jnp.float32,
    )


def local_stats(returns, task_bins, loss_mask, tasks):
    return pl.pallas_call(
        stats_kernel,
        out_shape=jax.ShapeDtypeStruct((SUBLANES, tasks), jnp.float32),
        name="task_stats",
    )(returns.reshape(1, -1), task_bins.reshape(1, -1), loss_mask.reshape(1, -1))


def on_device(hidden, value_weight, value_bias, returns, task_bins, loss_mask):
    dp, seq = lax.axis_size("dp"), lax.axis_size("seq")
    rounds = wide_rounds(dp, seq)
    rollouts = hidden.shape[0] * dp
    width, tasks = value_weight.shape
    states = hidden.reshape(-1, width)
    flat_returns = returns.reshape(-1)
    bins = task_bins.reshape(-1)
    bins_iota = jnp.arange(tasks, dtype=jnp.int32)
    stats = local_stats(returns, task_bins, loss_mask, tasks)
    chosen = (bins[:, None] == bins_iota).astype(jnp.float32)
    exchanges = small_rounds(dp * seq)
    parts = len(exchanges) - 1
    edges = [states.shape[0] * at // parts for at in range(parts + 1)]
    pieces = []
    for at, (stride, radix) in enumerate(exchanges):
        got = [shift(stats, (stride, stride), radix, by) for by in range(1, radix)]
        if at:
            rows = slice(edges[at - 1], edges[at])
            bias, stats = lax.optimization_barrier((value_bias, stats))
            scores = jnp.dot(states[rows], value_weight, preferred_element_type=jnp.float32)
            picked = jnp.sum((scores + bias) * chosen[rows], axis=-1)
            got, picked = lax.optimization_barrier((got, picked))
            pieces.append(picked)
        for piece in got:
            stats = stats + piece
    predicted = jnp.concatenate(pieces)
    counts, summed, squares = stats[0], stats[1], stats[2]
    floor_counts = jnp.maximum(counts, 1.0)
    means = summed / floor_counts
    second = squares - summed * means
    spread = jnp.sqrt(second / floor_counts + 0.1)
    deviation = flat_returns[:, None] - means
    targets = jnp.sum(chosen * (deviation / spread), axis=-1)
    valid = loss_mask.reshape(-1).astype(jnp.float32)
    slope = valid * jnp.clip(predicted - targets, -1.0, 1.0) / rollouts
    coefficient = chosen * slope[:, None]
    coefficient_low = coefficient.astype(jnp.bfloat16)
    bias_grad = jnp.sum(coefficient, axis=0)
    up, across = tasks // SUBLANES, width // LANES
    count = 2 if (up * across) % (2 * dp * seq) == 0 else 1
    chains = []
    for at in range(count):
        columns = slice(width * at // count, width * (at + 1) // count)
        part = lax.dot_general(
            states[:, columns],
            coefficient_low,
            (((0,), (0,)), ((), ())),
            preferred_element_type=jnp.float32,
        )
        part = lax.optimization_barrier(part).T
        part = part.reshape(up, SUBLANES, across // count, LANES).transpose(0, 2, 1, 3)
        chains.append(part.reshape(-1, SUBLANES, LANES))
    extra = jnp.zeros((SUBLANES, LANES), jnp.float32).at[0, :tasks].set(bias_grad)[None]
    chains, extra = all_sum(chains, extra, rounds)
    whole = []
    for tiles in chains:
        part = tiles.reshape(up, across // count, SUBLANES, LANES).transpose(0, 2, 1, 3)
        whole.append(part.reshape(tasks, width // count).T)
    return (targets.reshape(returns.shape), jnp.concatenate(whole, axis=0), extra[0, 0, :tasks])


def solution(mesh):
    placed = (P("dp", "seq", None), P(), P(), P("dp", "seq"), P("dp", "seq"), P("dp", "seq"))
    return jax.shard_map(
        on_device, mesh=mesh, in_specs=placed, out_specs=(P("dp", "seq"), P(), P()), check_vma=False
    )
```

```python
import jax
import jax.numpy as jnp
from jax import lax
from jax.experimental import pallas as pl
from jax.experimental.pallas import tpu as pltpu
from jax.sharding import PartitionSpec as P

LANES = 128
SUBLANES = 8
AXES = ("dp", "seq")


def factor(left, widest):
    return next(r for r in [widest, 2] + list(range(3, left + 1)) if left % r == 0)


def small_rounds(total):
    rounds, stride = [], 1
    while stride < total:
        radix = factor(total // stride, 2)
        rounds.append((stride, radix))
        stride *= radix
    return rounds


def row_edges(tokens, rounds):
    shares = [3,3,3,7]
    weights = [0] * (rounds - len(shares)) + shares if rounds >= len(shares) else [1] * rounds
    return [tokens * sum(weights[:at]) // sum(weights) for at in range(rounds + 1)]


def wide_rounds(dp, seq):
    rounds = []
    for first, left, plan in ((1, seq, (2, 2)), (seq, dp, (2, 4))):
        stride, at = first, 0
        while left > 1:
            radix = factor(left, plan[min(at, 1)])
            rounds.append((stride, radix))
            stride, left, at = stride * radix, left // radix, at + 1
    paired = [((stride, stride), radix) for stride, radix in rounds]
    ahead = [at for at, (stride, radix) in enumerate(rounds) if stride == seq]
    if len(rounds) > 2 and rounds[0] == (1, 2) and seq > 2 and ahead:
        one, other = rounds[1], rounds[ahead[0]]
        if one[1] == other[1] and one[0] != other[0]:
            paired[1] = ((one[0], other[0]), one[1])
            paired[ahead[0]] = ((other[0], one[0]), one[1])
            paired.insert(2, paired.pop(ahead[0]))
    return paired


def shift(value, strides, radix, by):
    pairs = []
    for source in range(lax.axis_size(AXES)):
        stride = strides[source % 2]
        digit = (source // stride) % radix
        pairs.append((source, source + ((digit + by) % radix - digit) * stride))
    return lax.ppermute(value, AXES, pairs)


def digit_of(strides, radix):
    here = lax.axis_index(AXES)
    stride = jnp.where(here % 2 == 0, strides[0], strides[1])
    return (here // stride) % radix


def scatter_round(tiles, extra, strides, radix):
    mine = digit_of(strides, radix)
    count = tiles.shape[0] // radix
    got = []
    for by in range(1, radix):
        part = lax.dynamic_slice_in_dim(tiles, ((mine + by) % radix) * count, count, 0)
        part = part if extra is None else jnp.concatenate([part, extra], axis=0)
        got.append(shift(part, strides, radix, by))
    tiles = lax.dynamic_slice_in_dim(tiles, mine * count, count, 0)
    for piece in got:
        tiles = tiles + piece[:count]
        extra = None if extra is None else extra + piece[count:]
    return tiles, extra


def gather_round(tiles, strides, radix):
    mine = digit_of(strides, radix)
    count = tiles.shape[0]
    got = [shift(tiles, strides, radix, by) for by in range(1, radix)]
    whole = jnp.zeros((count * radix,) + tiles.shape[1:], tiles.dtype)
    whole = lax.dynamic_update_slice_in_dim(whole, tiles, mine * count, 0)
    for by in range(1, radix):
        whole = lax.dynamic_update_slice_in_dim(whole, got[by - 1], ((mine - by) % radix) * count, 0)
    return whole


def all_sum(chains, extra, rounds):
    apart = min(3, len(rounds)) if len(chains) > 1 else 0
    extras = [None] * (len(chains) - 1) + [extra]
    for strides, radix in rounds[:apart]:
        both = [scatter_round(tiles, more, strides, radix) for tiles, more in zip(chains, extras)]
        chains, extras = [one[0] for one in both], [one[1] for one in both]
    extra = extras[-1]
    count = chains[0].shape[0]
    tiles = jnp.concatenate(chains, axis=0)
    for strides, radix in rounds[apart:]:
        tiles, extra = scatter_round(tiles, extra, strides, radix)
    for strides, radix in reversed(rounds[apart:]):
        tiles = gather_round(tiles, strides, radix)
    chains = [tiles[at * count:(at + 1) * count] for at in range(len(chains))]
    for strides, radix in reversed(rounds[:apart]):
        chains = [gather_round(tiles, strides, radix) for tiles in chains]
    return chains, extra


def stats_kernel(returns_ref, bins_ref, mask_ref, out_ref):
    rows, tasks = out_ref.shape
    tokens = returns_ref.shape[1]
    value = returns_ref[...]
    task = lax.broadcasted_iota(jnp.int32, (tasks, tokens), 0)
    onehot = (task == bins_ref[...]) & (mask_ref[...] != 0)
    row = lax.broadcasted_iota(jnp.int32, (rows, tokens), 0)
    terms = jnp.where(row == 0, 1.0, jnp.where(row == 1, value, jnp.where(row == 2, value * value, 0.0)))
    out_ref[...] = lax.dot_general(
        terms,
        jnp.where(onehot, 1.0, 0.0),
        (((1,), (1,)), ((), ())),
        precision=lax.Precision.HIGHEST,
        preferred_element_type=jnp.float32,
    )


def local_stats(returns, task_bins, loss_mask, tasks):
    return pl.pallas_call(
        stats_kernel,
        out_shape=pltpu.VMEM((SUBLANES, tasks), jnp.float32),
        name="task_stats",
    )(returns.reshape(1, -1), task_bins.reshape(1, -1), loss_mask.reshape(1, -1))


def on_device(hidden, value_weight, value_bias, returns, task_bins, loss_mask):
    dp, seq = lax.axis_size("dp"), lax.axis_size("seq")
    rounds = wide_rounds(dp, seq)
    rollouts = hidden.shape[0] * dp
    width, tasks = value_weight.shape
    states = hidden.reshape(-1, width)
    flat_returns = returns.reshape(-1)
    bins = task_bins.reshape(-1)
    bins_iota = jnp.arange(tasks, dtype=jnp.int32)
    stats = local_stats(returns, task_bins, loss_mask, tasks)
    chosen = (bins[:, None] == bins_iota).astype(jnp.float32)
    exchanges = small_rounds(dp * seq)
    tokens = states.shape[0]
    edges = row_edges(tokens, len(exchanges))
    pieces = []
    for at, (stride, radix) in enumerate(exchanges):
        got = [shift(stats, (stride, stride), radix, by) for by in range(1, radix)]
        rows = slice(edges[at], edges[at + 1])
        if rows.start < rows.stop:
            bias, stats = lax.optimization_barrier((value_bias, stats))
            scores = jnp.dot(states[rows], value_weight, preferred_element_type=jnp.float32)
            picked = jnp.sum((scores + bias) * chosen[rows], axis=-1)
            got, picked = lax.optimization_barrier((got, picked))
            pieces.append(picked)
        for piece in got:
            stats = stats + piece
    predicted = jnp.concatenate(pieces)
    counts, summed, squares = stats[0], stats[1], stats[2]
    floor_counts = jnp.maximum(counts, 1.0)
    means = summed / floor_counts
    second = squares - summed * means
    spread = jnp.sqrt(second / floor_counts + 0.1)
    deviation = flat_returns[:, None] - means
    targets = jnp.sum(chosen * (deviation / spread), axis=-1)
    valid = loss_mask.reshape(-1).astype(jnp.float32)
    slope = valid * jnp.clip(predicted - targets, -1.0, 1.0) / rollouts
    coefficient = chosen * slope[:, None]
    coefficient_low = coefficient.astype(jnp.bfloat16)
    bias_grad = jnp.sum(coefficient, axis=0)
    up, across = tasks // SUBLANES, width // LANES
    count = 2 if (up * across) % (2 * dp * seq) == 0 else 1
    chains = []
    for at in range(count):
        columns = slice(width * at // count, width * (at + 1) // count)
        part = lax.dot_general(
            states[:, columns],
            coefficient_low,
            (((0,), (0,)), ((), ())),
            preferred_element_type=jnp.float32,
        )
        part = lax.optimization_barrier(part).T
        part = part.reshape(up, SUBLANES, across // count, LANES).transpose(0, 2, 1, 3)
        chains.append(part.reshape(-1, SUBLANES, LANES))
    extra = jnp.zeros((SUBLANES, LANES), jnp.float32).at[0, :tasks].set(bias_grad)[None]
    chains, extra = all_sum(chains, extra, rounds)
    whole = []
    for tiles in chains:
        part = tiles.reshape(up, across // count, SUBLANES, LANES).transpose(0, 2, 1, 3)
        whole.append(part.reshape(tasks, width // count).T)
    return (targets.reshape(returns.shape), jnp.concatenate(whole, axis=0), extra[0, 0, :tasks])


def solution(mesh):
    placed = (P("dp", "seq", None), P(), P(), P("dp", "seq"), P("dp", "seq"), P("dp", "seq"))
    return jax.shard_map(
        on_device, mesh=mesh, in_specs=placed, out_specs=(P("dp", "seq"), P(), P()), check_vma=False
    )
```
